256 devices in a mesh: dp: 32 (over z, x_lo, core), row: 4 (over y), col: 2 (over x_hi).
Axes of the slice: x: 4 (x_hi: 2, x_lo: 2; x = x_hi * 2 + x_lo), y: 4, z: 8, core: 2. Of those that a mesh axis runs over, the one named last changes fastest.
Arguments:
- latents: bfloat16 [32768, 2048], P(('dp', 'col'), 'row'), parts along dimension 0, may hold values from -64 to 64
- norm_gain: float32 [65536], P(('dp', 'row')), parts along dimension 0, may hold values from 0.1 to 1.9
- q_weight: bfloat16 [65536, 2048], P(('dp', 'row'), 'col'), parts along dimension 0, may hold values from -1 to 1
- k_weight: bfloat16 [65536, 2048], P(('dp', 'row'), 'col'), parts along dimension 0, may hold values from -1 to 1
- v_weight: bfloat16 [65536, 2048], P(('dp', 'row'), 'col'), parts along dimension 0, may hold values from -0.125 to 0.125
- out_weight: bfloat16 [65536, 2048], P(('dp', 'col'), 'row'), parts along dimension 0, may hold values from -0.5 to 0.5
Outputs:
- attended: bfloat16 [32768, 2048], P(('dp', 'col'), 'row'), parts along dimension 0
The draws below stay inside these ranges and needn't reach their ends.
There are 32 independent parts, one for each index of `dp`. The reference program is written for one: setup_inputs(seed, part) draws one part's arguments, and reference() takes and returns one part's arrays. A program takes and returns all parts, laid end to end along the dimension named above; each array names one. Nothing has to cross between parts.
All inputs are finite; a program needn't handle non-finite values.
Results may differ from the reference program's by a relative error of at most 0.03.
Values may be sent and summed in bfloat16 or wider, within the bound.
No kernel may reach another device: no remote copies, remote signals or barrier semaphores. Data moves between devices by JAX's collectives and lax.ppermute only.
A program may use at most 64 MiB of HBM per device.

```python
import jax
import jax.numpy as jnp
from jax import lax

HEADS = 16
HEAD_DIM = 128
D = 2048
LATENTS = 1024
N_ROW = 4
N_COL = 2


def draw_latents(key, part):
    noise = jnp.clip(jax.random.normal(jax.random.fold_in(key, 1), (LATENTS, D), jnp.float32), -6.0, 6.0)
    ramp = jnp.arange(D, dtype=jnp.float32) / D
    values = noise * (3.0 ** ramp)[None, :]
    return jnp.clip(values, -64.0, 64.0).astype(jnp.bfloat16)


def projection(key, salt):
    base = jnp.clip(jax.random.normal(jax.random.fold_in(key, salt), (D, D), jnp.float32), -6.0, 6.0)
    return base * jnp.sqrt(2.0 / D)


def draw_q_weight(key, part):
    values = projection(key, 21)
    return jnp.clip(values, -1.0, 1.0).astype(jnp.bfloat16)


def draw_k_weight(key, part):
    values = projection(key, 22)
    return jnp.clip(values, -1.0, 1.0).astype(jnp.bfloat16)


def shard_levels(key, shape, split, low, largest):
    gain = 1.0
    for position, blocks in split:
        draws = jax.random.uniform(jax.random.fold_in(jax.random.fold_in(key, 6), position), (blocks,), jnp.float32, low / len(split), largest / len(split))
        gain = gain * jnp.repeat(jnp.exp(draws), shape[position] // blocks).reshape((-1,) + (1,) * (len(shape) - 1 - position))
    return gain


def centred(own_key, shape, scale, limit, cuts=(), held_as=jnp.bfloat16):
    gain = shard_levels(own_key, shape, cuts, -0.22, 0.18) if cuts else 1.0
    result = jax.random.normal(own_key, shape, jnp.float32) * scale * gain
    return jnp.minimum(jnp.maximum(result, -limit), limit).astype(held_as)


def setup_inputs(seed: int = 0, part: int = 0) -> dict:
    key_of = jax.random.split(jax.random.key(seed), 7)
    part_splits = jax.random.split(jax.random.fold_in(key_of[6], part), 7)
    return {
        "latents": draw_latents(jax.random.fold_in(jax.random.fold_in(key_of[6], part), 71), part),
        "norm_gain": jnp.clip(1.0 + 0.18 * jax.random.normal(part_splits[1], (D,), jnp.float32), 0.1, 1.9),
        "q_weight": draw_q_weight(jax.random.fold_in(jax.random.fold_in(key_of[6], part), 71), part),
        "k_weight": draw_k_weight(jax.random.fold_in(jax.random.fold_in(key_of[6], part), 71), part),
        "v_weight": centred(part_splits[4], (D, D), D ** -0.5, 0.125, ((0, 4), (1, 2))),
        "out_weight": centred(part_splits[5], (D, D), (D // 16) ** -0.5, 0.5, ((0, 2), (1, 4))),
    }


def blocked_sum(left, weight, pieces):
    width = left.shape[1] // pieces
    acc = jnp.zeros((left.shape[0], weight.shape[1]), jnp.float32)
    for index in range(pieces):
        part = jnp.dot(left[:, index * width:(index + 1) * width].astype(jnp.float32), weight[index * width:(index + 1) * width, :].astype(jnp.float32), preferred_element_type=jnp.float32)
        part = lax.optimization_barrier(part.astype(jnp.bfloat16))
        acc = acc + part.astype(jnp.float32)
    return acc.astype(jnp.bfloat16)

def reference(latents, norm_gain, q_weight, k_weight, v_weight, out_weight):
    wide = latents.astype(jnp.float32)
    total = lax.optimization_barrier(jnp.sum(wide * wide, axis=1))
    normed = (wide * lax.rsqrt(total / D + 1e-06)[:, None] * norm_gain[None, :]).astype(jnp.bfloat16)
    query = blocked_sum(normed, q_weight, N_ROW)
    keys = blocked_sum(normed, k_weight, N_ROW)
    values = blocked_sum(normed, v_weight, N_ROW)
    query3 = query.astype(jnp.float32).reshape(LATENTS, HEADS, HEAD_DIM)
    keys3 = keys.astype(jnp.float32).reshape(LATENTS, HEADS, HEAD_DIM)
    values3 = values.astype(jnp.float32).reshape(LATENTS, HEADS, HEAD_DIM)
    scores = jnp.einsum('qhd,khd->hqk', query3, keys3) / jnp.sqrt(jnp.float32(HEAD_DIM))
    peak = lax.optimization_barrier(jnp.max(scores, axis=2, keepdims=True))
    weights = jnp.exp(scores - peak)
    denom = lax.optimization_barrier(jnp.sum(weights, axis=2))
    rounded = weights.astype(jnp.bfloat16).astype(jnp.float32)
    mixed = jnp.einsum('hqk,khd->hqd', rounded, values3) / denom[:, :, None]
    mixed = jnp.transpose(mixed, (1, 0, 2)).reshape(LATENTS, D).astype(jnp.bfloat16)
    return blocked_sum(mixed, out_weight, N_COL)
```

```python
import functools

import jax
import jax.numpy as jnp
from jax import lax
from jax.experimental import pallas as pl
from jax.experimental.pallas import tpu as pltpu
from jax.sharding import PartitionSpec as P

HEAD_DIM = 128
D = 2048
BF16 = jnp.bfloat16
F32 = jnp.float32

P1 = [(0, 1), (1, 0), (2, 3), (3, 2)]
P2 = [(1, 2), (2, 1), (3, 0), (0, 3)]
OPP = [(0, 2), (1, 3), (2, 0), (3, 1)]
COL = [(0, 1), (1, 0)]
LOG2E = 1.4426950408889634


def dot(a, b):
    return jnp.dot(a, b, preferred_element_type=F32)


def project(head, target, pairs, gain, weights, arrived, out_dtype):
    tokens, width = pairs[0][0].shape

    def body(target_ref, gain_ref, q_ref, k_ref, v_ref, arrived_ref, *refs):
        out_ref = refs[-1]
        weight = jnp.concatenate([q_ref[...], k_ref[...], v_ref[...]], axis=1)
        there = arrived_ref[...]
        for index in range(len(pairs)):
            near = (refs[2 * index][...].astype(F32) * gain_ref[...]).astype(BF16)
            far = refs[2 * index + 1][...]
            value = dot(near, weight) + dot(far, there)
            out_ref[index * tokens : (index + 1) * tokens, :] = value.astype(out_dtype)

    whole = lambda shape: pl.BlockSpec(shape, lambda i, t: (0, 0))
    column = pl.BlockSpec((width, HEAD_DIM), lambda i, t: (0, 2 * t[0] + head))
    count = tokens * len(pairs)
    return pl.pallas_call(
        body,
        grid_spec=pltpu.PrefetchScalarGridSpec(
            num_scalar_prefetch=1,
            grid=(1,),
            in_specs=[whole((1, width)), column, column, column, whole(arrived.shape)]
            + [whole((tokens, width))] * (2 * len(pairs)),
            out_specs=whole((count, 3 * HEAD_DIM)),
        ),
        out_shape=jax.ShapeDtypeStruct((count, 3 * HEAD_DIM), out_dtype),
        cost_estimate=pl.CostEstimate(
            flops=2 * count * 2 * width * 3 * HEAD_DIM,
            bytes_accessed=count * width * 4 + 4 * width * 3 * HEAD_DIM,
            transcendentals=0,
        ),
        name="project",
    )(target.reshape(1), gain, *weights, arrived, *[block for pair in pairs for block in pair])


def attend(kept, far_own, far_other, scale):
    half = far_own.shape[0]
    block = 256

    def body(kept_ref, own_ref, other_ref, scale_ref, out_other_ref, out_own_ref, q_ref, k_ref, v_ref):
        for index, far_ref in enumerate((own_ref, other_ref)):
            rows = slice(index * half, (index + 1) * half)
            factor = jnp.broadcast_to(scale_ref[:, rows], (HEAD_DIM, half)).T
            value = kept_ref[rows, :] + far_ref[...].astype(F32)
            q_ref[rows, :] = (
                value[:, :HEAD_DIM] * (factor * (LOG2E / HEAD_DIM**0.5))
            ).astype(BF16)
            k_ref[rows, :] = (value[:, HEAD_DIM : 2 * HEAD_DIM] * factor).astype(BF16)
            v_ref[rows, :] = (value[:, 2 * HEAD_DIM :] * factor).astype(BF16)
        for start in list(range(half, 2 * half, block)) + list(range(0, half, block)):
            scores = lax.dot_general(
                q_ref[start : start + block, :],
                k_ref[...],
                (((1,), (1,)), ((), ())),
                preferred_element_type=F32,
            )
            weights = jnp.exp2(scores - jnp.max(scores, axis=1, keepdims=True))
            denom = jnp.sum(weights, axis=1, keepdims=True)
            mixed = (dot(weights.astype(BF16), v_ref[...]) / denom).astype(BF16)
            if start >= half:
                out_other_ref[start - half : start - half + block, :] = mixed
            else:
                out_own_ref[start : start + block, :] = mixed

    out = jax.ShapeDtypeStruct((half, HEAD_DIM), BF16)
    return pl.pallas_call(
        body,
        out_shape=(out, out),
        scratch_shapes=[pltpu.VMEM((2 * half, HEAD_DIM), BF16)] * 3,
        cost_estimate=pl.CostEstimate(
            flops=4 * 4 * half * half * HEAD_DIM * 2,
            bytes_accessed=2 * half * 3 * HEAD_DIM * 6,
            transcendentals=4 * half * half,
        ),
        name="attend",
    )(kept, far_own, far_other, scale)


def output_product(order, pieces, out_weight, extra, out_dtype):
    tokens = pieces[0][0].shape[0]
    columns = out_weight.shape[1]

    def body(order_ref, weight_ref, *refs):
        out_ref = refs[-1]
        total = refs[-2][...].astype(F32) if extra is not None else None
        for index in range(len(pieces)):
            left = jnp.concatenate([refs[2 * index][...], refs[2 * index + 1][...]], axis=1)
            start = pl.multiple_of(order_ref[index] * (2 * HEAD_DIM), 2 * HEAD_DIM)
            term = dot(left, weight_ref[pl.ds(start, 2 * HEAD_DIM), :])
            total = term if total is None else total + term
        out_ref[...] = total.astype(out_dtype)

    whole = lambda shape: pl.BlockSpec(shape, lambda i, t: (0, 0))
    operands = [block for pair in pieces for block in pair] + ([extra] if extra is not None else [])
    return pl.pallas_call(
        body,
        grid_spec=pltpu.PrefetchScalarGridSpec(
            num_scalar_prefetch=1,
            grid=(1,),
            in_specs=[whole(out_weight.shape)] + [whole(x.shape) for x in operands],
            out_specs=whole((tokens, columns)),
        ),
        out_shape=jax.ShapeDtypeStruct((tokens, columns), out_dtype),
        cost_estimate=pl.CostEstimate(
            flops=2 * tokens * columns * 2 * HEAD_DIM * len(pieces),
            bytes_accessed=4 * tokens * columns + out_weight.size * 2,
            transcendentals=0,
        ),
        name="output_product",
    )(order, out_weight, *operands)


def per_device(latents, norm_gain, q_weight, k_weight, v_weight, out_weight):
    send = lambda value, axis, pairs: lax.ppermute(value, axis, pairs)
    me = lax.axis_index("row")
    first, second, across = me ^ 1, 3 - me, me ^ 2
    gain = norm_gain[None, :]
    weights = (q_weight, k_weight, v_weight)

    def block_for(target, head):
        start = (2 * target + head) * HEAD_DIM
        parts = [lax.dynamic_slice_in_dim(w, start, HEAD_DIM, 1) for w in weights]
        return (jnp.concatenate(parts, axis=1).astype(F32) * norm_gain[:, None]).astype(BF16)

    own = latents
    own1 = send(own, "row", P1)
    own2 = send(own, "row", P2)
    other = send(own, "col", COL)
    pass0 = send(block_for(across, 0), "row", P1)
    pass1 = send(block_for(across, 1), "row", P2)
    stay0 = send(block_for(first, 0), "row", P1)
    stay1 = send(block_for(second, 1), "row", P2)
    other1 = send(own1, "col", COL)
    other2 = send(own2, "col", COL)

    far0_own = send(project(0, second, [(own, own1)], gain, weights, pass0, BF16), "row", P2)
    far1_own = send(project(1, first, [(own, own2)], gain, weights, pass1, BF16), "row", P1)
    far0_other = send(project(0, second, [(other, other1)], gain, weights, pass0, BF16), "row", P2)
    far1_other = send(project(1, first, [(other, other2)], gain, weights, pass1, BF16), "row", P1)

    square = lambda x: jnp.sum(jnp.square(x.astype(F32)), axis=1)
    pair_sum = jnp.concatenate([square(own) + square(own1), square(other) + square(other1)])
    total = pair_sum + send(pair_sum, "row", P2)
    scale = lax.rsqrt(total / D + 1e-06)[None, :]

    kept0 = project(0, me, [(own, own1), (other, other1)], gain, weights, stay0, F32)
    kept1 = project(1, me, [(own, own2), (other, other2)], gain, weights, stay1, F32)

    other_mixed0, own_mixed0 = attend(kept0, far0_own, far0_other, scale)
    other_mixed1, own_mixed1 = attend(kept1, far1_own, far1_other, scale)

    order = jnp.stack([me, first, second, across])

    def from_all(value):
        return [value, send(value, "row", P1), send(value, "row", P2), send(value, "row", OPP)]

    pieces_other = list(zip(from_all(other_mixed0), from_all(other_mixed1)))
    term = output_product(order, pieces_other, out_weight, None, BF16)
    pieces_own = list(zip(from_all(own_mixed0), from_all(own_mixed1)))
    arrived = send(term, "col", COL)
    return output_product(order, pieces_own, out_weight, arrived, BF16)


def solution(mesh):
    return jax.shard_map(
        per_device,
        mesh=mesh,
        in_specs=(
            P(("dp", "col"), "row"),
            P(("dp", "row")),
            P(("dp", "row"), "col"),
            P(("dp", "row"), "col"),
            P(("dp", "row"), "col"),
            P(("dp", "col"), "row"),
        ),
        out_specs=P(("dp", "col"), "row"),
        check_vma=False,
    )
```

```python
import jax
import jax.numpy as jnp
from jax import lax
from jax.experimental import pallas as pl
from jax.experimental.pallas import tpu as pltpu
from jax.sharding import PartitionSpec as P


HEAD_DIM = 128
D = 2048
BF16 = jnp.bfloat16
F32 = jnp.float32

P1 = [(0, 1), (1, 0), (2, 3), (3, 2)]
P2 = [(1, 2), (2, 1), (3, 0), (0, 3)]
OPP = [(0, 2), (1, 3), (2, 0), (3, 1)]
COL = [(0, 1), (1, 0)]
LOG2E = 1.4426950408889634
FIRST_MIB = 61


def ring():
    me = lax.axis_index("row")
    return me, me ^ 1, 3 - me, me ^ 2


ME, FIRST, SECOND, ACROSS = range(4)


def dot(a, b):
    return jnp.dot(a, b, preferred_element_type=F32)


def params(mebibytes):
    return pltpu.CompilerParams(vmem_limit_bytes=mebibytes * 2**20)


VMEM = pl.BlockSpec(memory_space=pltpu.VMEM)
HBM = pl.BlockSpec(memory_space=pltpu.HBM)


PAIR = 2 * HEAD_DIM


def columns_of(ref, start, count):
    return ref[:, pl.ds(pl.multiple_of(start, HEAD_DIM), count)]


def gained(near_ref, gain_ref):
    return (near_ref[...].astype(F32) * gain_ref[...]).astype(BF16)


def local_call(body, shapes, operands, flops, mebibytes=10, in_specs=None, scratch=(), exps=0):
    outs = [jax.ShapeDtypeStruct(shape, dtype) for shape, dtype in shapes]
    results = pl.pallas_call(
        body,
        in_specs=in_specs or [VMEM] * len(operands),
        out_specs=[VMEM] * len(outs),
        out_shape=outs,
        scratch_shapes=list(scratch),
        cost_estimate=pl.CostEstimate(
            flops=flops,
            bytes_accessed=sum(x.size * x.dtype.itemsize for x in list(operands) + outs),
            transcendentals=exps,
        ),
        compiler_params=params(mebibytes),
    )(*operands)
    return results if len(outs) > 1 else results[0]


def first_queries(near, gain, q_weight):
    tokens, width = near.shape

    def body(gain_ref, near_ref, q_ref, out_ref, here, held, sems):
        place = ring()
        copies = [pltpu.make_async_copy(near_ref, here, sems.at[0])]
        for slot, target in enumerate((ACROSS, SECOND)):
            start = pl.multiple_of(PAIR * place[target], PAIR)
            copies.append(
                pltpu.make_async_copy(
                    q_ref.at[:, pl.ds(start, PAIR)],
                    held.at[:, slot * PAIR : (slot + 1) * PAIR],
                    sems.at[slot + 1],
                )
            )
        for copy in copies:
            copy.start()
        copies[0].wait()
        block = gained(here, gain_ref)
        for slot in range(2):
            copies[slot + 1].wait()
            cut = slice(slot * PAIR, (slot + 1) * PAIR)
            out_ref[:, cut] = dot(block, held[:, cut]).astype(BF16)

    return local_call(
        body,
        [((tokens, 2 * PAIR), BF16)],
        (gain, near, q_weight),
        4 * tokens * width * PAIR,
        FIRST_MIB,
        [VMEM, HBM, HBM],
        [
            pltpu.VMEM((tokens, width), BF16),
            pltpu.VMEM((width, 2 * PAIR), BF16),
            pltpu.SemaphoreType.DMA((3,)),
        ],
    )


def folded(gain, k_weight, v_weight):
    width = k_weight.shape[0]

    def body(gain_ref, k_ref, v_ref, pass_ref, stay0_ref, stay1_ref):
        place = ring()
        factor = jnp.broadcast_to(gain_ref[...], (HEAD_DIM, width)).T
        for head in range(2):
            for which, ref in enumerate((k_ref, v_ref)):
                for target, out_ref, start in (
                    (ACROSS, pass_ref, head * PAIR),
                    (FIRST, (stay0_ref, stay1_ref)[head], 0),
                ):
                    block = columns_of(ref, PAIR * place[target] + head * HEAD_DIM, HEAD_DIM)
                    start = start + which * HEAD_DIM
                    out_ref[:, start : start + HEAD_DIM] = (block.astype(F32) * factor).astype(BF16)

    return local_call(
        body,
        [((width, 2 * PAIR), BF16), ((width, PAIR), BF16), ((width, PAIR), BF16)],
        (gain, k_weight, v_weight),
        8 * width * PAIR,
    )


def queries(targets, near, gain, q_weight, addend, out_dtype):
    tokens, width = near.shape
    extra = [] if addend is None else [addend[0]]

    def body(gain_ref, near_ref, q_ref, *refs):
        place = ring()
        here = gained(near_ref, gain_ref)
        for slot, target in enumerate(targets):
            value = dot(here, columns_of(q_ref, PAIR * place[target], PAIR))
            if extra:
                value = value + refs[0][:, addend[1] * PAIR : (addend[1] + 1) * PAIR].astype(F32)
            refs[-1][:, slot * PAIR : (slot + 1) * PAIR] = value.astype(out_dtype)

    return local_call(
        body,
        [((tokens, PAIR * len(targets)), out_dtype)],
        (gain, near, q_weight, *extra),
        2 * tokens * width * PAIR * len(targets),
    )


def keys_values(head, target, place_of_head, pairs, gain, k_weight, v_weight, arrived, out_dtype):
    tokens, width = pairs[0][0].shape

    def body(gain_ref, k_ref, v_ref, arrived_ref, *refs):
        start = PAIR * ring()[target] + head * HEAD_DIM
        weight = jnp.concatenate(
            [columns_of(k_ref, start, HEAD_DIM), columns_of(v_ref, start, HEAD_DIM)], axis=1
        )
        there = arrived_ref[:, place_of_head * PAIR : (place_of_head + 1) * PAIR]
        for index in range(len(pairs)):
            value = dot(gained(refs[2 * index], gain_ref), weight) + dot(refs[2 * index + 1][...], there)
            refs[-1][index * tokens : (index + 1) * tokens, :] = value.astype(out_dtype)

    return local_call(
        body,
        [((tokens * len(pairs), PAIR), out_dtype)],
        (gain, k_weight, v_weight, arrived, *[block for pair in pairs for block in pair]),
        4 * tokens * width * PAIR * len(pairs),
    )


def attend(head, q_own, q_other, kept, far_own, far_other, scale, beside):
    half = far_own.shape[0]
    block = 256
    offset = 0 if beside is None else HEAD_DIM
    operands = [scale, *q_own, *q_other, kept, far_own, far_other]
    operands += [] if beside is None else [beside]

    def body(scale_ref, qa_ref, qb_ref, qc_ref, qd_ref, kept_ref, own_ref, other_ref, *refs):
        out_other_ref, out_own_ref, q_ref, k_ref, v_ref = refs[-5:]
        if beside is not None:
            out_own_ref[:, :HEAD_DIM] = refs[0][...]
        cut = slice(head * HEAD_DIM, (head + 1) * HEAD_DIM)
        for index, (first_ref, second_ref, far_ref) in enumerate(
            ((qa_ref, qb_ref, own_ref), (qc_ref, qd_ref, other_ref))
        ):
            rows = slice(index * half, (index + 1) * half)
            factor = jnp.broadcast_to(scale_ref[:, rows], (HEAD_DIM, half)).T
            query = first_ref[:, cut].astype(F32) + second_ref[:, cut].astype(F32)
            value = kept_ref[rows, :] + far_ref[...].astype(F32)
            q_ref[rows, :] = (query * (factor * (LOG2E / HEAD_DIM**0.5))).astype(BF16)
            k_ref[rows, :] = (value[:, :HEAD_DIM] * factor).astype(BF16)
            v_ref[rows, :] = (value[:, HEAD_DIM:] * factor).astype(BF16)
        for start in list(range(half, 2 * half, block)) + list(range(0, half, block)):
            scores = lax.dot_general(
                q_ref[start : start + block, :],
                k_ref[...],
                (((1,), (1,)), ((), ())),
                preferred_element_type=F32,
            )
            weights = jnp.exp2(scores - jnp.max(scores, axis=1, keepdims=True))
            denom = jnp.sum(weights, axis=1, keepdims=True)
            mixed = (dot(weights.astype(BF16), v_ref[...]) / denom).astype(BF16)
            if start >= half:
                out_other_ref[start - half : start - half + block, :] = mixed
            else:
                out_own_ref[start : start + block, offset:] = mixed

    return local_call(
        body,
        [((half, HEAD_DIM), BF16), ((half, HEAD_DIM + offset), BF16)],
        operands,
        16 * half * half * HEAD_DIM,
        14,
        scratch=[pltpu.VMEM((2 * half, HEAD_DIM), BF16)] * 3,
        exps=4 * half * half,
    )


def output_product(terms, weights, extra, out_dtype):
    tokens = terms[0][0].shape[0]
    columns = sum(x.shape[1] for x in weights[0])
    bounds = [0]
    for pieces in weights:
        bounds.append(bounds[-1] + len(pieces))
    operands = [x for pieces in weights for x in pieces] + [term[0] for term in terms]
    operands += [] if extra is None else [extra]

    def body(*refs):
        spot = ring()
        piece_refs = refs[bounds[-1] : bounds[-1] + len(terms)]

        def operand(index):
            _, place, which, head, source = terms[index]
            rows = pl.ds(pl.multiple_of((2 * spot[source] + head) * HEAD_DIM, HEAD_DIM), HEAD_DIM)
            parts = [ref[rows, :] for ref in refs[bounds[which] : bounds[which + 1]]]
            return (
                piece_refs[index][:, place * HEAD_DIM : (place + 1) * HEAD_DIM],
                parts[0] if len(parts) == 1 else jnp.concatenate(parts, axis=1),
            )

        total = None if extra is None else refs[-2][...]
        for index in range(0, len(terms), 2):
            (left, top), (right, bottom) = operand(index), operand(index + 1)
            term = dot(
                jnp.concatenate([left, right], axis=1), jnp.concatenate([top, bottom], axis=0)
            )
            total = term if total is None else total + term
        refs[-1][...] = total.astype(out_dtype)

    return local_call(
        body, [((tokens, columns), out_dtype)], operands, 2 * tokens * columns * HEAD_DIM * len(terms), 12
    )


def sublayer(latents, norm_gain, q_weight, k_weight, v_weight, out_weight):
    gain = norm_gain[None, :]
    own = latents
    own1 = lax.ppermute(own, "row", P1)
    other = lax.ppermute(own, "col", COL)

    q_own = lax.ppermute(first_queries(own, gain, q_weight), "row", P2)
    both = (ACROSS, SECOND)
    q_other = lax.ppermute(queries(both, other, gain, q_weight, None, BF16), "row", P2)
    end_own = lax.ppermute(queries((FIRST,), own, gain, q_weight, (q_own, 0), BF16), "row", P1)
    end_other = lax.ppermute(queries((FIRST,), other, gain, q_weight, (q_other, 0), BF16), "row", P1)
    kept_q_own = queries((ME,), own, gain, q_weight, (q_own, 1), F32)
    kept_q_other = queries((ME,), other, gain, q_weight, (q_other, 1), F32)

    pass_block, stay_block0, stay_block1 = folded(gain, k_weight, v_weight)
    passed = lax.ppermute(pass_block, "row", P1)
    stay0 = lax.ppermute(stay_block0, "row", P1)
    stay1 = lax.ppermute(stay_block1, "row", P1)
    other1 = lax.ppermute(own1, "col", COL)

    def partial(head, target, place, pairs, arrived, out_dtype):
        return keys_values(head, target, place, pairs, gain, k_weight, v_weight, arrived, out_dtype)

    def sent_partial(head, pair):
        value = partial(head, SECOND, head, [pair], passed, BF16)
        return lax.ppermute(value, "row", P2)

    far0_own = sent_partial(0, (own, own1))
    far0_other = sent_partial(0, (other, other1))
    far1_own = sent_partial(1, (own, own1))
    far1_other = sent_partial(1, (other, other1))
    all_pairs = [(own, own1), (other, other1)]
    kept0 = partial(0, ME, 0, all_pairs, stay0, F32)
    kept1 = partial(1, ME, 0, all_pairs, stay1, F32)

    square = lambda x: jnp.sum(jnp.square(x.astype(F32)), axis=1)
    total = jnp.concatenate([square(own) + square(own1), square(other) + square(other1)])
    total = total + lax.ppermute(total, "row", P2)
    scale = lax.rsqrt(total / D + 1e-06)[None, :]

    def from_all(value):
        return [value, lax.ppermute(value, "row", P1), lax.ppermute(value, "row", P2), lax.ppermute(value, "row", OPP)]

    q_parts = ((kept_q_own, end_own), (kept_q_other, end_other))
    other0, own0 = attend(0, *q_parts, kept0, far0_own, far0_other, scale, None)
    partner0 = lax.ppermute(other0, "col", COL)
    own0_all = from_all(own0)
    other1_mixed, middle = attend(1, *q_parts, kept1, far1_own, far1_other, scale, partner0)
    partner1 = lax.ppermute(other1_mixed, "col", COL)
    middle_all = from_all(middle)
    partner1_all = from_all(partner1)

    half = out_weight.shape[1] // 2
    here = [out_weight]
    there = [lax.ppermute(out_weight[:, :half], "col", COL), lax.ppermute(out_weight[:, half:], "col", COL)]
    terms = [(x, 0, 0, 0, source) for source, x in enumerate(own0_all)]
    total = output_product(terms, [here], None, F32)
    terms = [(x, 0, 1, 0, source) for source, x in enumerate(middle_all)]
    terms += [(x, 1, 0, 1, source) for source, x in enumerate(middle_all)]
    total = output_product(terms, [here, there], total, F32)
    terms = [(x, 0, 0, 1, source) for source, x in enumerate(partner1_all)]
    return output_product(terms, [there], total, BF16)


def solution(mesh):
    return jax.shard_map(
        sublayer,
        mesh=mesh,
        in_specs=(
            P(("dp", "col"), "row"),
            P(("dp", "row")),
            P(("dp", "row"), "col"),
            P(("dp", "row"), "col"),
            P(("dp", "row"), "col"),
            P(("dp", "col"), "row"),
        ),
        out_specs=P(("dp", "col"), "row"),
        check_vma=False,
    )
```

```python
import jax
import jax.numpy as jnp
from jax import lax
from jax.experimental import pallas as pl
from jax.experimental.pallas import tpu as pltpu
from jax.sharding import PartitionSpec as P


HEAD_DIM = 128
D = 2048
BF16 = jnp.bfloat16
F32 = jnp.float32

P1 = [(0, 1), (1, 0), (2, 3), (3, 2)]
P2 = [(1, 2), (2, 1), (3, 0), (0, 3)]
OPP = [(0, 2), (1, 3), (2, 0), (3, 1)]
COL = [(0, 1), (1, 0)]
LOG2E = 1.4426950408889634
FIRST_MIB = 63
SUM_ROWS = 16


def ring():
    me = lax.axis_index("row")
    return me, me ^ 1, 3 - me, me ^ 2


ME, FIRST, SECOND, ACROSS = range(4)


def dot(a, b):
    return jnp.dot(a, b, preferred_element_type=F32)


def params(mebibytes):
    return pltpu.CompilerParams(vmem_limit_bytes=mebibytes * 2**20)


VMEM = pl.BlockSpec(memory_space=pltpu.VMEM)
HBM = pl.BlockSpec(memory_space=pltpu.HBM)


PAIR = 2 * HEAD_DIM


def columns_of(ref, start, count):
    return ref[:, pl.ds(pl.multiple_of(start, HEAD_DIM), count)]


def gained(near_ref, gain_ref):
    return (near_ref[...].astype(F32) * gain_ref[...]).astype(BF16)


def local_call(body, shapes, operands, flops, mebibytes=10, in_specs=None, scratch=(), exps=0):
    outs = [jax.ShapeDtypeStruct(shape, dtype) for shape, dtype in shapes]
    results = pl.pallas_call(
        body,
        in_specs=in_specs or [VMEM] * len(operands),
        out_specs=[VMEM] * len(outs),
        out_shape=outs,
        scratch_shapes=list(scratch),
        cost_estimate=pl.CostEstimate(
            flops=flops,
            bytes_accessed=sum(x.size * x.dtype.itemsize for x in list(operands) + outs),
            transcendentals=exps,
        ),
        compiler_params=params(mebibytes),
    )(*operands)
    return results if len(outs) > 1 else results[0]


def first_queries(near, gain, q_weight):
    tokens, width = near.shape

    def body(gain_ref, near_ref, q_ref, out_ref, here, held, sems):
        place = ring()
        copies = [pltpu.make_async_copy(near_ref, here, sems.at[0])]
        for slot, target in enumerate((ACROSS, SECOND)):
            start = pl.multiple_of(PAIR * place[target], PAIR)
            copies.append(
                pltpu.make_async_copy(
                    q_ref.at[:, pl.ds(start, PAIR)],
                    held.at[:, slot * PAIR : (slot + 1) * PAIR],
                    sems.at[slot + 1],
                )
            )
        for copy in copies:
            copy.start()
        copies[0].wait()
        block = gained(here, gain_ref)
        for slot in range(2):
            copies[slot + 1].wait()
            cut = slice(slot * PAIR, (slot + 1) * PAIR)
            out_ref[:, cut] = dot(block, held[:, cut]).astype(BF16)

    return local_call(
        body,
        [((tokens, 2 * PAIR), BF16)],
        (gain, near, q_weight),
        4 * tokens * width * PAIR,
        FIRST_MIB,
        [VMEM, HBM, HBM],
        [
            pltpu.VMEM((tokens, width), BF16),
            pltpu.VMEM((width, 2 * PAIR), BF16),
            pltpu.SemaphoreType.DMA((3,)),
        ],
    )


def folded(gain, k_weight, v_weight):
    width = k_weight.shape[0]

    def body(gain_ref, k_ref, v_ref, pass_ref, stay_ref):
        place = ring()
        factor = jnp.broadcast_to(gain_ref[...], (HEAD_DIM, width)).T
        for head in range(2):
            for which, ref in enumerate((k_ref, v_ref)):
                start = head * PAIR + which * HEAD_DIM
                for target, out_ref in ((ACROSS, pass_ref), (FIRST, stay_ref)):
                    block = columns_of(ref, PAIR * place[target] + head * HEAD_DIM, HEAD_DIM)
                    out_ref[:, start : start + HEAD_DIM] = (block.astype(F32) * factor).astype(BF16)

    return local_call(
        body,
        [((width, 2 * PAIR), BF16), ((width, 2 * PAIR), BF16)],
        (gain, k_weight, v_weight),
        8 * width * PAIR,
    )


def queries(targets, near, gain, q_weight, addend, out_dtype):
    tokens, width = near.shape
    extra = [] if addend is None else [addend[0]]

    def body(gain_ref, near_ref, q_ref, *refs):
        place = ring()
        here = gained(near_ref, gain_ref)
        for slot, target in enumerate(targets):
            value = dot(here, columns_of(q_ref, PAIR * place[target], PAIR))
            if extra:
                value = value + refs[0][:, addend[1] * PAIR : (addend[1] + 1) * PAIR].astype(F32)
            refs[-1][:, slot * PAIR : (slot + 1) * PAIR] = value.astype(out_dtype)

    return local_call(
        body,
        [((tokens, PAIR * len(targets)), out_dtype)],
        (gain, near, q_weight, *extra),
        2 * tokens * width * PAIR * len(targets),
    )


def squares(ref):
    wide = ref[...].astype(F32)
    return jnp.sum(wide * wide, axis=1, keepdims=True)


def as_row(column):
    return jnp.broadcast_to(column, (column.shape[0], HEAD_DIM)).T[:1, :]


def keys_values(head, target, place_of_head, pairs, gain, k_weight, v_weight, arrived, out_dtype, sums):
    tokens, width = pairs[0][0].shape
    count = tokens * len(pairs)

    def body(gain_ref, k_ref, v_ref, arrived_ref, *refs):
        start = PAIR * ring()[target] + head * HEAD_DIM
        weight = jnp.concatenate(
            [columns_of(k_ref, start, HEAD_DIM), columns_of(v_ref, start, HEAD_DIM)], axis=1
        )
        there = arrived_ref[:, place_of_head * PAIR : (place_of_head + 1) * PAIR]
        out_ref = refs[2 * len(pairs)]
        rows = []
        for index in range(len(pairs)):
            near_ref, far_ref = refs[2 * index], refs[2 * index + 1]
            value = dot(gained(near_ref, gain_ref), weight) + dot(far_ref[...], there)
            out_ref[index * tokens : (index + 1) * tokens, :] = value.astype(out_dtype)
            if sums:
                row = as_row(squares(near_ref) + squares(far_ref))
                refs[-1][:, index * tokens : (index + 1) * tokens] = row
                rows += [row[:, cut : cut + PAIR] for cut in range(0, tokens, PAIR)]
        if sums:
            rest = jnp.concatenate(rows, axis=0)
            terms = []
            for _ in range(3):
                terms.append(rest.astype(BF16))
                rest = rest - terms[-1].astype(F32)
            blank = jnp.zeros((SUM_ROWS - 3 * len(rows), PAIR), F32)
            wide = [term.astype(F32) for term in terms] + [blank]
            out_ref[count:, :] = jnp.concatenate(wide, axis=0).astype(out_dtype)

    shapes = [((count + (SUM_ROWS if sums else 0), PAIR), out_dtype)]
    if sums:
        shapes.append(((1, count), F32))
    return local_call(
        body,
        shapes,
        (gain, k_weight, v_weight, arrived, *[block for pair in pairs for block in pair]),
        4 * tokens * width * PAIR * len(pairs),
    )


def attend(head, q_kept, q_end, kept, far, near_sums, far_sums, beside):
    count = kept.shape[0]
    half = count // 2
    block = 512
    offset = 0 if beside is None else HEAD_DIM
    groups = [q_kept, q_end, far, near_sums, far_sums, [kept], [] if beside is None else [beside]]
    operands = [x for group in groups for x in group]

    def body(*refs):
        refs = list(refs)
        qk_refs, qe_refs, far_refs, near_sums_refs, far_sums_refs, (kept_ref,), beside_refs = [
            [refs.pop(0) for _ in group] for group in groups
        ]
        out_other_ref, out_own_ref, q_ref, k_ref, v_ref = refs
        if beside_refs:
            out_own_ref[:, :HEAD_DIM] = beside_refs[0][...]
        cut = slice(head * HEAD_DIM, (head + 1) * HEAD_DIM)
        lines = half // PAIR
        for index in range(2):
            coded = far_sums_refs[index][half : half + SUM_ROWS, :].astype(F32)
            sums = coded[:lines, :] + coded[lines : 2 * lines, :] + coded[2 * lines : 3 * lines, :]
            for part in range(lines):
                near = slice(part * PAIR, (part + 1) * PAIR)
                rows = slice(index * half + part * PAIR, index * half + (part + 1) * PAIR)
                total = near_sums_refs[index][:, near] + sums[part : part + 1, :]
                scale = lax.rsqrt(total / D + 1e-06)
                factor = jnp.broadcast_to(scale, (HEAD_DIM, PAIR)).T
                query = qk_refs[index][near, cut].astype(F32) + qe_refs[index][near, cut].astype(F32)
                if len(far_refs) == 2:
                    arrived = far_refs[index][near, :]
                else:
                    arrived = far_refs[0][rows, :]
                value = kept_ref[rows, :] + arrived.astype(F32)
                q_ref[rows, :] = (query * (factor * (LOG2E / HEAD_DIM**0.5))).astype(BF16)
                k_ref[rows, :] = (value[:, :HEAD_DIM] * factor).astype(BF16)
                v_ref[rows, :] = (value[:, HEAD_DIM:] * factor).astype(BF16)
        for start in list(range(half, 2 * half, block)) + list(range(0, half, block)):
            scores = lax.dot_general(
                q_ref[start : start + block, :],
                k_ref[...],
                (((1,), (1,)), ((), ())),
                preferred_element_type=F32,
            )
            weights = jnp.exp2(scores - jnp.max(scores, axis=1, keepdims=True))
            denom = jnp.sum(weights, axis=1, keepdims=True)
            mixed = (dot(weights.astype(BF16), v_ref[...]) / denom).astype(BF16)
            if start >= half:
                out_other_ref[start - half : start - half + block, :] = mixed
            else:
                out_own_ref[start : start + block, offset:] = mixed

    return local_call(
        body,
        [((half, HEAD_DIM), BF16), ((half, HEAD_DIM + offset), BF16)],
        operands,
        16 * half * half * HEAD_DIM,
        14,
        scratch=[pltpu.VMEM((count, HEAD_DIM), BF16)] * 3,
        exps=4 * half * half,
    )


def output_product(terms, weights, extra, out_dtype):
    tokens = terms[0][0].shape[0]
    columns = sum(x.shape[1] for x in weights[0])
    bounds = [0]
    for pieces in weights:
        bounds.append(bounds[-1] + len(pieces))
    operands = [x for pieces in weights for x in pieces] + [term[0] for term in terms]
    operands += [] if extra is None else [extra]

    def body(*refs):
        spot = ring()
        piece_refs = refs[bounds[-1] : bounds[-1] + len(terms)]

        def operand(index):
            _, place, which, head, source = terms[index]
            rows = pl.ds(pl.multiple_of((2 * spot[source] + head) * HEAD_DIM, HEAD_DIM), HEAD_DIM)
            parts = [ref[rows, :] for ref in refs[bounds[which] : bounds[which + 1]]]
            return (
                piece_refs[index][:, place * HEAD_DIM : (place + 1) * HEAD_DIM],
                parts[0] if len(parts) == 1 else jnp.concatenate(parts, axis=1),
            )

        total = None if extra is None else refs[-2][...]
        for index in range(0, len(terms), 2):
            (left, top), (right, bottom) = operand(index), operand(index + 1)
            term = dot(
                jnp.concatenate([left, right], axis=1), jnp.concatenate([top, bottom], axis=0)
            )
            total = term if total is None else total + term
        refs[-1][...] = total.astype(out_dtype)

    return local_call(
        body,
        [((tokens, columns), out_dtype)],
        operands,
        2 * tokens * columns * HEAD_DIM * len(terms),
        12,
    )


def sublayer(latents, norm_gain, q_weight, k_weight, v_weight, out_weight):
    gain = norm_gain[None, :]
    own = latents
    own1 = lax.ppermute(own, "row", P1)
    other = lax.ppermute(own, "col", COL)

    q_own = lax.ppermute(first_queries(own, gain, q_weight), "row", P2)
    both = (ACROSS, SECOND)
    q_other = lax.ppermute(queries(both, other, gain, q_weight, None, BF16), "row", P2)
    end_own = lax.ppermute(queries((FIRST,), own, gain, q_weight, (q_own, 0), BF16), "row", P1)
    end_other = lax.ppermute(
        queries((FIRST,), other, gain, q_weight, (q_other, 0), BF16), "row", P1
    )
    kept_q_own = queries((ME,), own, gain, q_weight, (q_own, 1), F32)
    kept_q_other = queries((ME,), other, gain, q_weight, (q_other, 1), F32)

    pass_block, stay_block = folded(gain, k_weight, v_weight)
    passed = lax.ppermute(pass_block, "row", P1)
    stay = lax.ppermute(stay_block, "row", P1)
    other1 = lax.ppermute(own1, "col", COL)
    pairs = [(own, own1), (other, other1)]

    def partial(head, target, place, pairs, arrived, out_dtype, sums=False):
        return keys_values(
            head, target, place, pairs, gain, k_weight, v_weight, arrived, out_dtype, sums
        )

    value, sums_own = partial(0, SECOND, 0, pairs[:1], passed, BF16, True)
    far0_own = lax.ppermute(value, "row", P2)
    value, sums_other = partial(0, SECOND, 0, pairs[1:], passed, BF16, True)
    far0_other = lax.ppermute(value, "row", P2)
    far0 = [far0_own, far0_other]
    far1 = [lax.ppermute(partial(1, SECOND, 1, pairs, passed, BF16), "row", P2)]
    near_sums = [sums_own, sums_other]
    kept0 = partial(0, ME, 0, pairs, stay, F32)
    kept1 = partial(1, ME, 1, pairs, stay, F32)

    def from_all(value):
        return [
            value,
            lax.ppermute(value, "row", P1),
            lax.ppermute(value, "row", P2),
            lax.ppermute(value, "row", OPP),
        ]

    q_parts = ((kept_q_own, kept_q_other), (end_own, end_other))
    other0, own0 = attend(0, *q_parts, kept0, far0, near_sums, far0, None)
    partner0 = lax.ppermute(other0, "col", COL)
    own0_all = from_all(own0)
    other1_mixed, middle = attend(1, *q_parts, kept1, far1, near_sums, far0, partner0)
    partner1 = lax.ppermute(other1_mixed, "col", COL)
    middle_all = from_all(middle)
    partner1_all = from_all(partner1)

    here = [out_weight]
    there = [lax.ppermute(out_weight, "col", COL)]
    terms = [(x, 0, 0, 0, source) for source, x in enumerate(own0_all)]
    total = output_product(terms, [here], None, F32)
    terms = [(x, 0, 1, 0, source) for source, x in enumerate(middle_all)]
    terms += [(x, 1, 0, 1, source) for source, x in enumerate(middle_all)]
    total = output_product(terms, [here, there], total, F32)
    terms = [(x, 0, 0, 1, source) for source, x in enumerate(partner1_all)]
    return output_product(terms, [there], total, BF16)


def solution(mesh):
    return jax.shard_map(
        sublayer,
        mesh=mesh,
        in_specs=(
            P(("dp", "col"), "row"),
            P(("dp", "row")),
            P(("dp", "row"), "col"),
            P(("dp", "row"), "col"),
            P(("dp", "row"), "col"),
            P(("dp", "col"), "row"),
        ),
        out_specs=P(("dp", "col"), "row"),
        check_vma=False,
    )
```

```python
import jax
import jax.numpy as jnp
from jax import lax
from jax.experimental import pallas as pl
from jax.experimental.pallas import tpu as pltpu
from jax.sharding import PartitionSpec as P


HEAD_DIM = 128
D = 2048
BF16 = jnp.bfloat16
F32 = jnp.float32

P1 = [(0, 1), (1, 0), (2, 3), (3, 2)]
P2 = [(1, 2), (2, 1), (3, 0), (0, 3)]
OPP = [(0, 2), (1, 3), (2, 0), (3, 1)]
COL = [(0, 1), (1, 0)]
LOG2E = 1.4426950408889634
FIRST_MIB = 63
SUM_ROWS = 16


def ring():
    me = lax.axis_index("row")
    return me, me ^ 1, 3 - me, me ^ 2


ME, FIRST, SECOND, ACROSS = range(4)


def dot(a, b):
    return jnp.dot(a, b, preferred_element_type=F32)


def params(mebibytes):
    return pltpu.CompilerParams(vmem_limit_bytes=mebibytes * 2**20)


VMEM = pl.BlockSpec(memory_space=pltpu.VMEM)
HBM = pl.BlockSpec(memory_space=pltpu.HBM)


PAIR = 2 * HEAD_DIM


def columns_of(ref, start, count):
    return ref[:, pl.ds(pl.multiple_of(start, HEAD_DIM), count)]


def gained(near_ref, gain_ref):
    return (near_ref[...].astype(F32) * gain_ref[...]).astype(BF16)


def local_call(body, shapes, operands, flops, mebibytes=10, in_specs=None, scratch=(), exps=0, out_spec=VMEM):
    outs = [jax.ShapeDtypeStruct(shape, dtype) for shape, dtype in shapes]
    results = pl.pallas_call(
        body,
        in_specs=in_specs or [VMEM] * len(operands),
        out_specs=[out_spec] * len(outs),
        out_shape=outs,
        scratch_shapes=list(scratch),
        cost_estimate=pl.CostEstimate(
            flops=flops,
            bytes_accessed=sum(x.size * x.dtype.itemsize for x in list(operands) + outs),
            transcendentals=exps,
        ),
        compiler_params=params(mebibytes),
    )(*operands)
    return results if len(outs) > 1 else results[0]


def first_queries(near, gain, q_weight):
    tokens, width = near.shape

    def body(gain_ref, near_ref, q_ref, out_ref, here, held, ready, sems):
        place = ring()
        copies = [pltpu.make_async_copy(near_ref, here, sems.at[0])]
        for slot, target in enumerate((ACROSS, SECOND)):
            start = pl.multiple_of(PAIR * place[target], PAIR)
            copies.append(
                pltpu.make_async_copy(
                    q_ref.at[:, pl.ds(start, PAIR)],
                    held.at[:, slot * PAIR : (slot + 1) * PAIR],
                    sems.at[slot + 1],
                )
            )
        for copy in copies:
            copy.start()
        copies[0].wait()
        block = gained(here, gain_ref)
        for slot in range(2):
            copies[slot + 1].wait()
            cut = slice(slot * PAIR, (slot + 1) * PAIR)
            ready[:, cut] = dot(block, held[:, cut]).astype(BF16)
            copies.append(pltpu.make_async_copy(ready.at[:, cut], out_ref.at[:, cut], sems.at[slot + 3]))
            copies[-1].start()
        for copy in copies[3:]:
            copy.wait()

    return local_call(
        body,
        [((tokens, 2 * PAIR), BF16)],
        (gain, near, q_weight),
        4 * tokens * width * PAIR,
        FIRST_MIB,
        [VMEM, HBM, HBM],
        [
            pltpu.VMEM((tokens, width), BF16),
            pltpu.VMEM((width, 2 * PAIR), BF16),
            pltpu.VMEM((tokens, 2 * PAIR), BF16),
            pltpu.SemaphoreType.DMA((5,)),
        ],
        out_spec=HBM,
    )


def folded(gain, k_weight, v_weight):
    width = k_weight.shape[0]

    def body(gain_ref, k_ref, v_ref, pass_ref, stay_ref):
        place = ring()
        factor = jnp.broadcast_to(gain_ref[...], (HEAD_DIM, width)).T
        for head in range(2):
            for which, ref in enumerate((k_ref, v_ref)):
                start = head * PAIR + which * HEAD_DIM
                for target, out_ref in ((ACROSS, pass_ref), (FIRST, stay_ref)):
                    block = columns_of(ref, PAIR * place[target] + head * HEAD_DIM, HEAD_DIM)
                    out_ref[:, start : start + HEAD_DIM] = (block.astype(F32) * factor).astype(BF16)

    return local_call(
        body, [((width, 2 * PAIR), BF16), ((width, 2 * PAIR), BF16)], (gain, k_weight, v_weight), 8 * width * PAIR
    )


def queries(targets, near, gain, q_weight, addend, out_dtype):
    tokens, width = near.shape
    extra = [] if addend is None else [addend[0]]

    def body(gain_ref, near_ref, q_ref, *refs):
        place = ring()
        here = gained(near_ref, gain_ref)
        for slot, target in enumerate(targets):
            value = dot(here, columns_of(q_ref, PAIR * place[target], PAIR))
            if extra:
                value = value + refs[0][:, addend[1] * PAIR : (addend[1] + 1) * PAIR].astype(F32)
            refs[-1][:, slot * PAIR : (slot + 1) * PAIR] = value.astype(out_dtype)

    return local_call(
        body,
        [((tokens, PAIR * len(targets)), out_dtype)],
        (gain, near, q_weight, *extra),
        2 * tokens * width * PAIR * len(targets),
    )


def squares(ref):
    wide = ref[...].astype(F32)
    return jnp.sum(wide * wide, axis=1, keepdims=True)


def as_row(column):
    return jnp.broadcast_to(column, (column.shape[0], HEAD_DIM)).T[:1, :]


def keys_values(head, target, place_of_head, pairs, gain, k_weight, v_weight, arrived, out_dtype, sums):
    tokens, width = pairs[0][0].shape
    count = tokens * len(pairs)

    def body(gain_ref, k_ref, v_ref, arrived_ref, *refs):
        start = PAIR * ring()[target] + head * HEAD_DIM
        weight = jnp.concatenate(
            [columns_of(k_ref, start, HEAD_DIM), columns_of(v_ref, start, HEAD_DIM)], axis=1
        )
        there = arrived_ref[:, place_of_head * PAIR : (place_of_head + 1) * PAIR]
        out_ref = refs[2 * len(pairs)]
        rows = []
        for index in range(len(pairs)):
            near_ref, far_ref = refs[2 * index], refs[2 * index + 1]
            value = dot(gained(near_ref, gain_ref), weight) + dot(far_ref[...], there)
            out_ref[index * tokens : (index + 1) * tokens, :] = value.astype(out_dtype)
            if sums:
                row = as_row(squares(near_ref) + squares(far_ref))
                refs[-1][:, index * tokens : (index + 1) * tokens] = row
                rows += [row[:, cut : cut + PAIR] for cut in range(0, tokens, PAIR)]
        if sums:
            rest = jnp.concatenate(rows, axis=0)
            terms = []
            for _ in range(3):
                terms.append(rest.astype(BF16))
                rest = rest - terms[-1].astype(F32)
            blank = jnp.zeros((SUM_ROWS - 3 * len(rows), PAIR), F32)
            wide = [term.astype(F32) for term in terms] + [blank]
            out_ref[count:, :] = jnp.concatenate(wide, axis=0).astype(out_dtype)

    shapes = [((count + (SUM_ROWS if sums else 0), PAIR), out_dtype)]
    if sums:
        shapes.append(((1, count), F32))
    return local_call(
        body,
        shapes,
        (gain, k_weight, v_weight, arrived, *[block for pair in pairs for block in pair]),
        4 * tokens * width * PAIR * len(pairs),
    )


def attend(head, q_kept, q_end, kept, far, near_sums, far_sums, beside):
    count = kept.shape[0]
    half = count // 2
    block = 512
    offset = 0 if beside is None else HEAD_DIM
    groups = [q_kept, q_end, far, near_sums, far_sums, [kept], [] if beside is None else [beside]]
    operands = [x for group in groups for x in group]

    def body(*refs):
        refs = list(refs)
        qk_refs, qe_refs, far_refs, near_sums_refs, far_sums_refs, (kept_ref,), beside_refs = [
            [refs.pop(0) for _ in group] for group in groups
        ]
        out_other_ref, out_own_ref, q_ref, k_ref, v_ref = refs
        if beside_refs:
            out_own_ref[:, :HEAD_DIM] = beside_refs[0][...]
        cut = slice(head * HEAD_DIM, (head + 1) * HEAD_DIM)
        lines = half // PAIR
        for index in range(2):
            coded = far_sums_refs[index][half : half + SUM_ROWS, :].astype(F32)
            sums = coded[:lines, :] + coded[lines : 2 * lines, :] + coded[2 * lines : 3 * lines, :]
            for part in range(lines):
                near = slice(part * PAIR, (part + 1) * PAIR)
                rows = slice(index * half + part * PAIR, index * half + (part + 1) * PAIR)
                total = near_sums_refs[index][:, near] + sums[part : part + 1, :]
                scale = lax.rsqrt(total / D + 1e-06)
                factor = jnp.broadcast_to(scale, (HEAD_DIM, PAIR)).T
                query = qk_refs[index][near, cut].astype(F32) + qe_refs[index][near, cut].astype(F32)
                if len(far_refs) == 2:
                    arrived = far_refs[index][near, :]
                else:
                    arrived = far_refs[0][rows, :]
                value = kept_ref[rows, :] + arrived.astype(F32)
                q_ref[rows, :] = (query * (factor * (LOG2E / HEAD_DIM**0.5))).astype(BF16)
                k_ref[rows, :] = (value[:, :HEAD_DIM] * factor).astype(BF16)
                v_ref[rows, :] = (value[:, HEAD_DIM:] * factor).astype(BF16)
        for start in list(range(half, 2 * half, block)) + list(range(0, half, block)):
            scores = lax.dot_general(
                q_ref[start : start + block, :],
                k_ref[...],
                (((1,), (1,)), ((), ())),
                preferred_element_type=F32,
            )
            weights = jnp.exp2(scores - jnp.max(scores, axis=1, keepdims=True))
            denom = jnp.sum(weights, axis=1, keepdims=True)
            mixed = (dot(weights.astype(BF16), v_ref[...]) / denom).astype(BF16)
            if start >= half:
                out_other_ref[start - half : start - half + block, :] = mixed
            else:
                out_own_ref[start : start + block, offset:] = mixed

    return local_call(
        body,
        [((half, HEAD_DIM), BF16), ((half, HEAD_DIM + offset), BF16)],
        operands,
        16 * half * half * HEAD_DIM,
        14,
        scratch=[pltpu.VMEM((count, HEAD_DIM), BF16)] * 3,
        exps=4 * half * half,
    )


def output_product(terms, weights, extra, out_dtype, last=False):
    tokens = terms[0][0].shape[0]
    columns = sum(x.shape[1] for x in weights[0])
    bounds = [0]
    for pieces in weights:
        bounds.append(bounds[-1] + len(pieces))
    operands = [x for pieces in weights for x in pieces] + [term[0] for term in terms]
    operands += [] if extra is None else [extra]

    def body(*refs):
        spot = ring()
        piece_refs = refs[bounds[-1] : bounds[-1] + len(terms)]

        def operand(index):
            _, place, which, head, source = terms[index]
            rows = pl.ds(pl.multiple_of((2 * spot[source] + head) * HEAD_DIM, HEAD_DIM), HEAD_DIM)
            parts = [ref[rows, :] for ref in refs[bounds[which] : bounds[which + 1]]]
            return (
                piece_refs[index][:, place * HEAD_DIM : (place + 1) * HEAD_DIM],
                parts[0] if len(parts) == 1 else jnp.concatenate(parts, axis=1),
            )

        out_ref = refs[bounds[-1] + len(terms) + (extra is not None)]
        steps = 2 if last else 1
        size = tokens // steps
        copies = []
        for step in range(steps):
            rows = slice(step * size, (step + 1) * size)
            total = None if extra is None else refs[bounds[-1] + len(terms)][rows, :]
            for index in range(0, len(terms), 2):
                (left, top), (right, bottom) = operand(index), operand(index + 1)
                term = dot(
                    jnp.concatenate([left[rows, :], right[rows, :]], axis=1),
                    jnp.concatenate([top, bottom], axis=0),
                )
                total = term if total is None else total + term
            if last:
                ready, sems = refs[-2:]
                ready[rows, :] = total.astype(out_dtype)
                copies.append(pltpu.make_async_copy(ready.at[rows], out_ref.at[rows], sems.at[step]))
                copies[-1].start()
            else:
                out_ref[...] = total.astype(out_dtype)
        for copy in copies:
            copy.wait()

    return local_call(
        body,
        [((tokens, columns), out_dtype)],
        operands,
        2 * tokens * columns * HEAD_DIM * len(terms),
        12,
        scratch=[pltpu.VMEM((tokens, columns), out_dtype), pltpu.SemaphoreType.DMA((2,))] if last else [],
        out_spec=HBM if last else VMEM,
    )


def sublayer(latents, norm_gain, q_weight, k_weight, v_weight, out_weight):
    gain = norm_gain[None, :]
    own = latents
    own1 = lax.ppermute(own, "row", P1)
    other = lax.ppermute(own, "col", COL)

    q_own = lax.ppermute(first_queries(own, gain, q_weight), "row", P2)
    both = (ACROSS, SECOND)
    q_other = lax.ppermute(queries(both, other, gain, q_weight, None, BF16), "row", P2)
    end_own = lax.ppermute(queries((FIRST,), own, gain, q_weight, (q_own, 0), BF16), "row", P1)
    end_other = lax.ppermute(queries((FIRST,), other, gain, q_weight, (q_other, 0), BF16), "row", P1)
    kept_q_own = queries((ME,), own, gain, q_weight, (q_own, 1), F32)
    kept_q_other = queries((ME,), other, gain, q_weight, (q_other, 1), F32)

    pass_block, stay_block = folded(gain, k_weight, v_weight)
    passed = lax.ppermute(pass_block, "row", P1)
    stay = lax.ppermute(stay_block, "row", P1)
    other1 = lax.ppermute(own1, "col", COL)
    pairs = [(own, own1), (other, other1)]

    def partial(head, target, place, pairs, arrived, out_dtype, sums=False):
        return keys_values(head, target, place, pairs, gain, k_weight, v_weight, arrived, out_dtype, sums)

    value, sums_own = partial(0, SECOND, 0, pairs[:1], passed, BF16, True)
    far0_own = lax.ppermute(value, "row", P2)
    value, sums_other = partial(0, SECOND, 0, pairs[1:], passed, BF16, True)
    far0_other = lax.ppermute(value, "row", P2)
    far0 = [far0_own, far0_other]
    far1 = [lax.ppermute(partial(1, SECOND, 1, pairs, passed, BF16), "row", P2)]
    near_sums = [sums_own, sums_other]
    kept0 = partial(0, ME, 0, pairs, stay, F32)
    kept1 = partial(1, ME, 1, pairs, stay, F32)

    def from_all(value):
        return [value, lax.ppermute(value, "row", P1), lax.ppermute(value, "row", P2), lax.ppermute(value, "row", OPP)]

    q_parts = ((kept_q_own, kept_q_other), (end_own, end_other))
    other0, own0 = attend(0, *q_parts, kept0, far0, near_sums, far0, None)
    partner0 = lax.ppermute(other0, "col", COL)
    own0_all = from_all(own0)
    other1_mixed, middle = attend(1, *q_parts, kept1, far1, near_sums, far0, partner0)
    partner1 = lax.ppermute(other1_mixed, "col", COL)
    middle_all = from_all(middle)
    partner1_all = from_all(partner1)

    here = [out_weight]
    there = [lax.ppermute(out_weight, "col", COL)]
    terms = [(x, 0, 0, 0, source) for source, x in enumerate(own0_all)]
    total = output_product(terms, [here], None, F32)
    terms = [(x, 0, 1, 0, source) for source, x in enumerate(middle_all)]
    terms += [(x, 1, 0, 1, source) for source, x in enumerate(middle_all)]
    total = output_product(terms, [here, there], total, F32)
    terms = [(x, 0, 0, 1, source) for source, x in enumerate(partner1_all)]
    return output_product(terms, [there], total, BF16, True)


def solution(mesh):
    return jax.shard_map(
        sublayer,
        mesh=mesh,
        in_specs=(
            P(("dp", "col"), "row"),
            P(("dp", "row")),
            P(("dp", "row"), "col"),
            P(("dp", "row"), "col"),
            P(("dp", "row"), "col"),
            P(("dp", "col"), "row"),
        ),
        out_specs=P(("dp", "col"), "row"),
        check_vma=False,
    )
```
